32 devices in a mesh: ta: 16 (over z, x, core), aa: 2 (over y).
Axes of the slice: x: 2, y: 2, z: 4, core: 2. Of those that a mesh axis runs over, the one named last changes fastest.
Arguments:
- voltages: bfloat16 [256, 393216], P('aa', 'ta'), may hold values from -6 to 6
- pfb_window: float32 [4, 8192], replicated, may hold values from -3 to 3
Outputs:
- visibilities: float32 [2048, 256, 512], P('ta', 'aa')
The draws below stay inside these ranges and needn't reach their ends.
All inputs are finite; a program needn't handle non-finite values.
Results may differ from the reference program's by a relative error of at most 0.0026.
Values may be sent and summed in bfloat16 or wider, within the bound.
A program may use at most 192 MiB of HBM per device.

```python
import math
import jax
import jax.numpy as jnp
from jax import lax

S = 256
NFFT = 8192
CH = 2048
TAPS = 4
FRAMES = 48
CH_OFF = 1024


def steps_of(rng, dims, pieces, least, high):
    gain = 1.0
    for axis_at, blocks in pieces:
        heights = jax.random.uniform(jax.random.fold_in(jax.random.fold_in(rng, 6), axis_at), (blocks,), jnp.float32, least / len(pieces), high / len(pieces))
        gain = gain * jnp.repeat(jnp.exp(heights), dims[axis_at] // blocks).reshape((-1,) + (1,) * (len(dims) - 1 - axis_at))
    return gain


def scatter_about(key, dims, scale, bound, cuts=(), held_as=jnp.bfloat16):
    values = scale * jax.random.normal(key, dims, jnp.float32)
    if cuts:
        values = values * steps_of(key, dims, cuts, -0.22, 0.18)
    return jnp.clip(values, -bound, bound).astype(held_as)


def setup_inputs(seed: int = 0) -> dict:
    streams_of = jax.random.split(jax.random.key(seed), 3)
    return {
        "voltages": scatter_about(streams_of[0], (S, FRAMES * NFFT), 1.0, 6.0, ((0, 2), (1, 16))),
        "pfb_window": scatter_about(streams_of[1], (TAPS, NFFT), 0.5, 3.0, (), jnp.float32),
    }


def reference(voltages, pfb_window):
    frames = voltages.shape[1] // NFFT
    padded = jnp.concatenate([jnp.zeros((S, (TAPS - 1) * NFFT), voltages.dtype), voltages], axis=1)
    window = pfb_window.astype(jnp.float32)

    def one_frame(frame_index):
        start_index = (frame_index * NFFT).astype(jnp.int32)
        samples = lax.dynamic_slice_in_dim(padded, start_index, TAPS * NFFT, 1)
        samples = samples.astype(jnp.float32).reshape(S, TAPS, NFFT)
        filtered = lax.optimization_barrier(jnp.sum(samples * window[None], axis=1))
        spectrum = jnp.fft.rfft(filtered, axis=1)[:, CH_OFF:CH_OFF + CH] / math.sqrt(NFFT)
        stacked = jnp.stack([jnp.real(spectrum), jnp.imag(spectrum)], axis=0).astype(jnp.float32)
        return jnp.transpose(stacked, (2, 0, 1)).astype(jnp.bfloat16)
    spectra = lax.map(one_frame, jnp.arange(frames, dtype=jnp.int32))
    spectra = jnp.transpose(spectra, (1, 0, 2, 3))
    scaling = 1.0 / math.sqrt(frames)
    blocks = spectra.reshape(CH // 16, 16, frames, 2, S)

    def one_block(channel_block):
        values = channel_block.astype(jnp.float32)
        swapped = jnp.stack([values[:, :, 1], -values[:, :, 0]], axis=2)
        left_rows = jnp.concatenate([values, swapped], axis=3)
        result = jnp.einsum('cfpi,cfpj->cij', left_rows, values) * scaling
        return jnp.concatenate([result[:, :S], result[:, S:]], axis=2)
    visible = lax.map(one_block, blocks)
    return visible.reshape(CH, S, 2 * S)
```

```python
import functools
import math

import jax
import jax.numpy as jnp
import numpy as np
from jax import lax
from jax.experimental import pallas as pl
from jax.experimental.pallas import tpu as pltpu
from jax.sharding import PartitionSpec as P

NFFT = 8192
CH = 2048
TAPS = 4
CH_OFF = 1024
RADIX = 32
INNER = NFFT // RADIX
BINS = CH // RADIX
HALF = RADIX // 2
LANES = 128
SIG_BLOCK = 16
LEFT = TAPS - 2
MESH = pl.DeviceIdType.MESH


def split_bf16(x):
    hi = jnp.asarray(x, jnp.bfloat16)
    return hi, (x - hi.astype(jnp.float32)).astype(jnp.bfloat16)


def stage_two_matrix():
    n2 = np.arange(INNER)[None, :]
    m = np.arange(BINS)[:, None] + CH_OFF // RADIX
    angle = 2.0 * np.pi * ((n2 * m) % INNER) / INNER
    mirror = 2.0 * np.pi * ((n2 * (m + 1)) % INNER) / INNER
    rows = [
        np.concatenate([np.cos(angle), np.sin(angle)], axis=1),
        np.concatenate([-np.sin(angle), np.cos(angle)], axis=1),
        np.concatenate([np.cos(mirror), -np.sin(mirror)], axis=1),
        np.concatenate([-np.sin(mirror), -np.cos(mirror)], axis=1),
    ]
    full = np.concatenate(rows, axis=0) / math.sqrt(NFFT)
    hi = full.astype(jnp.bfloat16)
    lo = (full - hi.astype(np.float64)).astype(jnp.bfloat16)
    return hi, lo


def twist_table():
    k = np.arange(HALF + 1)[:, None]
    n2 = np.arange(INNER)[None, :]
    angle = 2.0 * np.pi * (k * n2) / NFFT
    return np.stack([np.cos(angle), -np.sin(angle)]).astype(np.float32)


def rfft_list(x):
    n = len(x)
    if n == 2:
        return [(x[0] + x[1], None), (x[0] - x[1], None)]
    even, odd = rfft_list(x[0::2]), rfft_list(x[1::2])
    out = [None] * (n // 2 + 1)
    for k in range(n // 4 + 1):
        er, ei = even[k]
        our, oui = odd[k]
        if k == 0:
            out[0] = (er + our, None)
            out[n // 2] = (er - our, None)
        elif k == n // 4:
            out[k] = (er, -our)
        else:
            c = math.cos(2 * math.pi * k / n)
            s = math.sin(2 * math.pi * k / n)
            if 8 * k == n:
                tr, ti = (our + oui) * c, (oui - our) * c
            else:
                tr, ti = our * c + oui * s, oui * c - our * s
            out[k] = (er + tr, ei + ti)
            out[n // 2 - k] = (er - tr, ti - ei)
    return out


def channel_frame(signals, first, here_at, volts, win, twist, mat_hi, mat_lo, parts_s, spec_s, out):
    def block(step, carry):
        rows = pl.ds(pl.multiple_of(step * SIG_BLOCK, SIG_BLOCK), SIG_BLOCK)
        low_rows = pl.ds(pl.multiple_of(signals + step * SIG_BLOCK, SIG_BLOCK), SIG_BLOCK)
        for part in range(INNER // LANES):
            filtered = []
            for n1 in range(RADIX):
                cols = pl.ds(n1 * INNER + part * LANES, LANES)
                total = win[0:1, cols] * volts[first, rows, cols].astype(jnp.float32)
                for t in range(1, TAPS):
                    total = total + win[t : t + 1, cols] * volts[first + t, rows, cols].astype(jnp.float32)
                filtered.append(total)
            here = pl.ds(part * LANES, LANES)
            there = pl.ds(INNER + part * LANES, LANES)
            for k, (ar, ai) in enumerate(rfft_list(filtered)):
                if k == 0:
                    br, bi = ar, jnp.zeros_like(ar)
                else:
                    tr, ti = twist[0, k : k + 1, here], twist[1, k : k + 1, here]
                    if ai is None:
                        br, bi = ar * tr, ar * ti
                    else:
                        br, bi = ar * tr - ai * ti, ar * ti + ai * tr
                for value, cols in ((br, here), (bi, there)):
                    hi, lo = split_bf16(value)
                    parts_s[k, rows, cols] = hi
                    parts_s[k, low_rows, cols] = lo
        return carry

    lax.fori_loop(0, signals // SIG_BLOCK, block, 0)
    dims = (((1,), (1,)), ((), ()))

    def dot(a, b):
        return lax.dot_general(a, b, dims, preferred_element_type=jnp.float32)

    def put(value, k):
        spec_s[pl.ds(2 * k, BINS, stride=2 * RADIX), :] = value[:BINS]
        spec_s[pl.ds(2 * k + 1, BINS, stride=2 * RADIX), :] = value[BINS:]

    for k in range(HALF + 1):
        size = 2 * BINS if k in (0, HALF) else 4 * BINS
        a_hi, a_lo = mat_hi[:size, :], mat_lo[:size, :]
        both = dot(a_hi, parts_s[k])
        small = dot(a_lo, parts_s[k, :signals])
        res = both[:, :signals] + (both[:, signals:] + small)
        put(res[: 2 * BINS], k)
        if size > 2 * BINS:
            put(res[2 * BINS :], RADIX - k)

    flat = out.at[here_at].reshape(2 * CH, signals)

    def cast(i, carry):
        at = pl.ds(pl.multiple_of(i * 128, 128), 128)
        flat[at, :] = spec_s[at, :].astype(jnp.bfloat16)
        return carry

    lax.fori_loop(0, 2 * CH // 128, cast, 0)


def exchange_kernel(signals, frames, peers, vol, win, twist, mat_hi, mat_lo, grid_out,
                    volts, wmask, parts_s, spec_s, spec,
                    load_sem, halo_send, halo_recv, own_sem, send_sem, recv_sem, over_send, over_recv):
    ta, aa = lax.axis_index("ta"), lax.axis_index("aa")
    core = ta % 2
    last = peers - 1
    mine = CH // peers
    right, left = (ta + 1) % peers, (ta + last) % peers

    load = pltpu.make_async_copy
    loads = [
        load(vol.at[:, pl.ds(f * NFFT, NFFT)], volts.at[LEFT + f], load_sem.at[f])
        for f in range(frames)
    ]
    for copy in loads:
        copy.start()

    barrier = pltpu.get_barrier_semaphore()

    def greet(i, carry):
        pl.semaphore_signal(barrier, 1, device_id=((ta + i) % peers, aa), device_id_type=MESH)
        return carry

    lax.fori_loop(1, peers, greet, 0)
    pl.semaphore_signal(barrier, 1, device_id=(ta, 1 - aa), device_id_type=MESH)
    pl.semaphore_wait(barrier, peers)

    def to_right(slot):
        return pltpu.make_async_remote_copy(
            vol.at[:, pl.ds((frames - LEFT + slot) * NFFT, NFFT)], volts.at[slot],
            halo_send.at[slot], halo_recv.at[slot],
            device_id=(right, aa), device_id_type=MESH)

    to_left = pltpu.make_async_remote_copy(
        vol.at[:, pl.ds(0, NFFT)], volts.at[LEFT + frames],
        halo_send.at[LEFT], halo_recv.at[LEFT],
        device_id=(left, aa), device_id_type=MESH)

    @pl.when(ta < last)
    def _():
        for slot in reversed(range(LEFT)):
            to_right(slot).start()

    to_left.start()

    @pl.when(ta == 0)
    def _():
        def clear(i, carry):
            rows = pl.ds(pl.multiple_of(i * SIG_BLOCK, SIG_BLOCK), SIG_BLOCK)
            for slot in range(LEFT):
                volts[slot, rows, :] = jnp.zeros((SIG_BLOCK, NFFT), jnp.bfloat16)
            return carry

        lax.fori_loop(0, signals // SIG_BLOCK, clear, 0)

    for copy in loads:
        copy.wait()

    def send(step, frame, i):
        to = (ta + i) % peers
        return pltpu.make_async_remote_copy(
            spec.at[step, pl.ds(to * mine, mine)], grid_out.at[aa, :, frame * peers + ta],
            send_sem.at[frame, i], recv_sem.at[frame, i],
            device_id=(to, aa), device_id_type=MESH)

    def keep(step, frame):
        return load(spec.at[step, pl.ds(ta * mine, mine)], grid_out.at[aa, :, frame * peers + ta],
                    own_sem.at[frame])

    def over_own(step, frame):
        return pltpu.make_async_remote_copy(
            spec.at[step, pl.ds(ta * mine, mine)], grid_out.at[aa, :, frame * peers + ta],
            over_send.at[frame, 0], over_recv.at[frame, 0],
            device_id=(ta, 1 - aa), device_id_type=MESH)

    def arrival(frame, i):
        source = (ta + peers - i) % peers
        place = grid_out.at[aa, :, frame * peers + source]
        return pltpu.make_async_remote_copy(
            place, place, send_sem.at[frame, i], recv_sem.at[frame, i],
            device_id=(source, aa), device_id_type=MESH)

    def over(side, frame, i):
        source = (ta + peers - i) % peers
        place = grid_out.at[side, :, frame * peers + source]
        return pltpu.make_async_remote_copy(
            place, place, over_send.at[frame, i], over_recv.at[frame, i],
            device_id=(ta, 1 - aa), device_id_type=MESH)

    def outward(n):
        return peers // 2 + jnp.where(n % 2 == 0, n // 2, -((n + 1) // 2))

    def frame_at(step):
        return jnp.where(core == 0, frames - 1 - step, step)

    def one_step(step, carry):
        frame = frame_at(step)

        @pl.when((step == 0) & (core == 0) | (step == frames - 1) & (core == 1))
        def _():
            to_left.wait_recv()

        for slot in range(LEFT):
            when = jnp.where(core == 0, frames - 1 - slot, 0)

            @pl.when((step == when) & (ta > 0))
            def _():
                to_right(slot).wait_recv()

        first_tap = (ta == last) & (frame == frames - 1)
        keep_old = jnp.where(first_tap, 0.0, 1.0).astype(jnp.float32)
        wmask[0 : TAPS - 1, :] = win[0 : TAPS - 1, :] * keep_old
        wmask[TAPS - 1 : TAPS, :] = win[TAPS - 1 : TAPS, :]
        channel_frame(signals, frame, step, volts, wmask, twist, mat_hi, mat_lo, parts_s, spec_s, spec)

        def each(n, c):
            send(step, frame, outward(n)).start()
            return c

        lax.fori_loop(0, peers - 1, each, 0)
        over_own(step, frame).start()
        keep(step, frame).start()
        return carry

    lax.fori_loop(0, frames, one_step, 0)

    def forward(at, carry):
        step, n = at // (peers - 1), at % (peers - 1)
        i = outward(peers - 2 - n)
        source = (ta + peers - i) % peers
        frame = jnp.where(source % 2 == 0, frames - 1 - step, step)
        arrival(frame, i).wait_recv()
        over(aa, frame, i).start()
        return carry

    lax.fori_loop(0, frames * (peers - 1), forward, 0)

    def settle(step, carry):
        frame = frame_at(step)
        keep(step, frame).wait()
        over_own(step, frame).wait_send()
        over(1 - aa, frame, 0).wait_recv()

        def each(i, c):
            send(step, frame, i).wait_send()
            over(aa, frame, i).wait_send()
            over(1 - aa, frame, i).wait_recv()
            return c

        lax.fori_loop(1, peers, each, 0)
        return carry

    lax.fori_loop(0, frames, settle, 0)

    @pl.when(ta < last)
    def _():
        for slot in range(LEFT):
            to_right(slot).wait_send()

    to_left.wait_send()


def exchange(voltages, window, signals, frames, peers):
    mat_hi, mat_lo = stage_two_matrix()
    dma = pltpu.SemaphoreType.DMA
    vmem = pl.BlockSpec(memory_space=pltpu.VMEM)
    hbm = pl.BlockSpec(memory_space=pltpu.HBM)
    mine = CH // peers
    return pl.pallas_call(
        functools.partial(exchange_kernel, signals, frames, peers),
        out_shape=jax.ShapeDtypeStruct((2, mine, frames * peers, 2, signals), jnp.bfloat16),
        in_specs=[hbm, vmem, vmem, vmem, vmem],
        out_specs=hbm,
        scratch_shapes=[
            pltpu.VMEM((LEFT + frames + 1, signals, NFFT), jnp.bfloat16),
            pltpu.VMEM((TAPS, NFFT), jnp.float32),
            pltpu.VMEM((HALF + 1, 2 * signals, 2 * INNER), jnp.bfloat16),
            pltpu.VMEM((2 * CH, signals), jnp.float32),
            pltpu.VMEM((frames, CH, 2, signals), jnp.bfloat16),
            dma((frames,)),
            dma((LEFT + 1,)),
            dma((LEFT + 1,)),
            dma((frames,)),
            dma((frames, peers)),
            dma((frames, peers)),
            dma((frames, peers)),
            dma((frames, peers)),
        ],
        compiler_params=pltpu.CompilerParams(
            collective_id=0, has_side_effects=True, vmem_limit_bytes=48 * 1024 * 1024
        ),
    )(voltages, window, jnp.asarray(twist_table()), jnp.asarray(mat_hi), jnp.asarray(mat_lo))


def correlate_kernel(block, signals, scale, place, grid_in, out):
    side = place[0]
    rows = grid_in.shape[2]
    dims = (((0,), (0,)), ((), ()))
    even = lax.broadcasted_iota(jnp.int32, (rows, signals), 0) % 2 == 0
    for c in range(block):
        left = grid_in[side, c]
        wide = left.astype(jnp.float32)
        turned = jnp.where(even, pltpu.roll(wide, rows - 1, 0), -pltpu.roll(wide, 1, 0))
        both = jnp.concatenate([left, turned.astype(jnp.bfloat16)], axis=1)
        against = jnp.concatenate([grid_in[0, c], grid_in[1, c]], axis=1)
        res = lax.dot_general(both, against, dims, preferred_element_type=jnp.float32) * scale
        out[c, :, : 2 * signals] = res[:signals]
        out[c, :, 2 * signals :] = res[signals:]


def correlate(spectra, place, scale):
    _, channels, rows, signals = spectra.shape
    block = 16 if rows <= 128 else 8
    return pl.pallas_call(
        functools.partial(correlate_kernel, block, signals, scale),
        grid_spec=pltpu.PrefetchScalarGridSpec(
            num_scalar_prefetch=1,
            grid=(channels // block,),
            in_specs=[pl.BlockSpec((2, block, rows, signals), lambda i, p: (0, i, 0, 0))],
            out_specs=pl.BlockSpec((block, signals, 4 * signals), lambda i, p: (i, 0, 0)),
        ),
        out_shape=jax.ShapeDtypeStruct((channels, signals, 4 * signals), jnp.float32),
        compiler_params=pltpu.CompilerParams(
            dimension_semantics=("arbitrary",), vmem_limit_bytes=40 * 1024 * 1024
        ),
    )(place.astype(jnp.int32).reshape(1), spectra)


def per_device(voltages, pfb_window):
    signals, samples = voltages.shape
    frames = samples // NFFT
    peers = lax.axis_size("ta")
    assert lax.axis_size("aa") == 2 and frames >= TAPS - 1 and signals == LANES
    spectra = exchange(voltages, pfb_window, signals, frames, peers)
    spectra = spectra.reshape(2, CH // peers, frames * peers * 2, signals)
    scale = 1.0 / math.sqrt(frames * peers)
    return correlate(spectra, lax.axis_index("aa"), scale)


def solution(mesh):
    return jax.shard_map(
        per_device, mesh=mesh, in_specs=(P("aa", "ta"), P()), out_specs=P("ta", "aa", None),
        check_vma=False,
    )
```

```python
import functools
import math

import jax
import jax.numpy as jnp
import numpy as np
from jax import lax
from jax.experimental import pallas as pl
from jax.experimental.pallas import tpu as pltpu
from jax.sharding import PartitionSpec as P

NFFT = 8192
CH = 2048
TAPS = 4
CH_OFF = 1024
RADIX = 32
INNER = NFFT // RADIX
BINS = CH // RADIX
HALF = RADIX // 2
LANES = 128
SIG_BLOCK = 16
MESH = pl.DeviceIdType.MESH


def split_bf16(x):
    hi = jnp.asarray(x, jnp.bfloat16)
    return hi, (x - hi.astype(jnp.float32)).astype(jnp.bfloat16)


def stage_two_matrix():
    n2 = np.arange(INNER)[None, :]
    m = np.arange(BINS)[:, None] + CH_OFF // RADIX
    angle = 2.0 * np.pi * ((n2 * m) % INNER) / INNER
    mirror = 2.0 * np.pi * ((n2 * (m + 1)) % INNER) / INNER
    rows = [
        np.concatenate([np.cos(angle), np.sin(angle)], axis=1),
        np.concatenate([-np.sin(angle), np.cos(angle)], axis=1),
        np.concatenate([np.cos(mirror), -np.sin(mirror)], axis=1),
        np.concatenate([-np.sin(mirror), -np.cos(mirror)], axis=1),
    ]
    full = np.concatenate(rows, axis=0) / math.sqrt(NFFT)
    hi = full.astype(jnp.bfloat16)
    lo = (full - hi.astype(np.float64)).astype(jnp.bfloat16)
    return hi, lo


def twist_table():
    k = np.arange(HALF + 1)[:, None]
    n2 = np.arange(INNER)[None, :]
    angle = 2.0 * np.pi * (k * n2) / NFFT
    return np.stack([np.cos(angle), -np.sin(angle)]).astype(np.float32)


def rfft_list(x):
    n = len(x)
    if n == 2:
        return [(x[0] + x[1], None), (x[0] - x[1], None)]
    even, odd = rfft_list(x[0::2]), rfft_list(x[1::2])
    out = [None] * (n // 2 + 1)
    for k in range(n // 4 + 1):
        er, ei = even[k]
        our, oui = odd[k]
        if k == 0:
            out[0] = (er + our, None)
            out[n // 2] = (er - our, None)
        elif k == n // 4:
            out[k] = (er, -our)
        else:
            c = math.cos(2 * math.pi * k / n)
            s = math.sin(2 * math.pi * k / n)
            if 8 * k == n:
                tr, ti = (our + oui) * c, (oui - our) * c
            else:
                tr, ti = our * c + oui * s, oui * c - our * s
            out[k] = (er + tr, ei + ti)
            out[n // 2 - k] = (er - tr, ti - ei)
    return out


def pair(a, b, peers):
    total, bit = 0, 1
    while bit < peers:
        total = total + (a // bit + b // bit) % 2 * bit
        bit *= 2
    return total


def channel_frame(signals, volts, win, twist, mat_hi, mat_lo, parts_s, spec):
    taps = volts.shape[0]

    def block(step, carry):
        rows = pl.ds(pl.multiple_of(step * SIG_BLOCK, SIG_BLOCK), SIG_BLOCK)
        low_rows = pl.ds(pl.multiple_of(signals + step * SIG_BLOCK, SIG_BLOCK), SIG_BLOCK)
        for part in range(INNER // LANES):
            filtered = []
            for n1 in range(RADIX):
                cols = pl.ds(n1 * INNER + part * LANES, LANES)
                total = win[0:1, cols] * volts[0, rows, cols].astype(jnp.float32)
                for t in range(1, taps):
                    total = total + win[t : t + 1, cols] * volts[t, rows, cols].astype(jnp.float32)
                filtered.append(total)
            here = pl.ds(part * LANES, LANES)
            there = pl.ds(INNER + part * LANES, LANES)
            for k, (ar, ai) in enumerate(rfft_list(filtered)):
                if k == 0:
                    br, bi = ar, jnp.zeros_like(ar)
                else:
                    tr, ti = twist[0, k : k + 1, here], twist[1, k : k + 1, here]
                    if ai is None:
                        br, bi = ar * tr, ar * ti
                    else:
                        br, bi = ar * tr - ai * ti, ar * ti + ai * tr
                for value, cols in ((br, here), (bi, there)):
                    hi, lo = split_bf16(value)
                    parts_s[k, rows, cols] = hi
                    parts_s[k, low_rows, cols] = lo
        return carry

    lax.fori_loop(0, signals // SIG_BLOCK, block, 0)
    dims = (((1,), (1,)), ((), ()))

    def dot(a, b):
        return lax.dot_general(a, b, dims, preferred_element_type=jnp.float32)

    def put(value, k):
        spec[pl.ds(2 * k, BINS, stride=2 * RADIX), :] = value[:BINS]
        spec[pl.ds(2 * k + 1, BINS, stride=2 * RADIX), :] = value[BINS:]

    for k in range(HALF + 1):
        size = 2 * BINS if k in (0, HALF) else 4 * BINS
        a_hi, a_lo = mat_hi[:size, :], mat_lo[:size, :]
        both = dot(a_hi, parts_s[k])
        small = dot(a_lo, parts_s[k, :signals])
        res = both[:, :signals] + (both[:, signals:] + small)
        put(res[: 2 * BINS], k)
        if size > 2 * BINS:
            put(res[2 * BINS :], RADIX - k)


def exchange_kernel(signals, frames, peers, vol, win_in, twist_in, hi_in, lo_in, grid_out,
                    volts, win, twist, mat_hi, mat_lo, weff, parts_s, spec, give, take, take_wide, done,
                    const_sem, load_sem, give_send, give_recv, own_sem, send_sem, recv_sem, over_send, over_recv):
    ta, aa = lax.axis_index("ta"), lax.axis_index("aa")
    core, side = ta % 2, ta // 2 % 2
    last = peers - 1
    mine = CH // peers
    wide = 2 * mine
    half = peers // 2
    right, left = (ta + 1) % peers, (ta + last) % peers
    near = ta + 1 - 2 * core
    far = jnp.where(core == 0, left, right)

    copy = pltpu.make_async_copy
    consts = [
        copy(source, target, const_sem.at[slot])
        for slot, (source, target) in enumerate(
            ((win_in, win), (twist_in, twist), (hi_in, mat_hi), (lo_in, mat_lo)))
    ]
    loads = [
        copy(vol.at[:, pl.ds(f * NFFT, NFFT)], volts.at[f], load_sem.at[f]) for f in range(frames)
    ]
    for one in consts + loads:
        one.start()

    barrier = pltpu.get_barrier_semaphore()

    def greet(i, carry):
        pl.semaphore_signal(barrier, 1, device_id=(pair(ta, i, peers), aa), device_id_type=MESH)
        return carry

    lax.fori_loop(1, peers, greet, 0)
    pl.semaphore_signal(barrier, 1, device_id=(ta, 1 - aa), device_id_type=MESH)
    for one in consts + loads:
        one.wait()
    pl.semaphore_wait(barrier, peers)

    def edge(kind):
        return jnp.where(core == kind, ta, right)

    def owner(kind, j):
        return jnp.where(kind == 0, j // 2 * 4 + 2 * side + j % 2, 2 * j + core)

    def give_far(f):
        return pltpu.make_async_remote_copy(
            give.at[f], take.at[f], give_send.at[f], give_recv.at[f],
            device_id=(far, aa), device_id_type=MESH)

    def give_near(f):
        return pltpu.make_async_remote_copy(
            spec.at[frames + f].reshape(half, 2, wide, signals).at[:, 1 - core], take_wide.at[f],
            give_send.at[frames + f], give_recv.at[frames + f],
            device_id=(near, aa), device_id_type=MESH)

    def place(which, boundary, f):
        return grid_out.at[which, :, boundary * frames + f]

    def block(kind, f, j):
        return done.at[kind * frames + f, pl.ds(j * mine, mine)]

    def send(kind, f, j):
        return pltpu.make_async_remote_copy(
            block(kind, f, j), place(aa, edge(kind), f),
            send_sem.at[kind * frames + f, j], recv_sem.at[edge(kind), f],
            device_id=(owner(kind, j), aa), device_id_type=MESH)

    def own_block(kind):
        return jnp.where(kind == 0, ta // 4 * 2 + core, ta // 2)

    def keep(kind, f):
        return copy(block(kind, f, own_block(kind)), place(aa, edge(kind), f), own_sem.at[kind * frames + f])

    def over_own(kind, f):
        return pltpu.make_async_remote_copy(
            block(kind, f, own_block(kind)), place(aa, edge(kind), f),
            over_send.at[edge(kind), f], over_recv.at[edge(kind), f],
            device_id=(ta, 1 - aa), device_id_type=MESH)

    def maker(boundary):
        before = (boundary + last) % peers
        by_core = before + core
        by_side = jnp.where(boundary // 2 % 2 == side, boundary, before)
        return jnp.where(boundary % 2 == 1, by_core, by_side)

    def arrival(boundary, f):
        here = place(aa, boundary, f)
        return pltpu.make_async_remote_copy(
            here, here, send_sem.at[0, 0], recv_sem.at[boundary, f],
            device_id=(maker(boundary), aa), device_id_type=MESH)

    def over(which, boundary, f):
        here = place(which, boundary, f)
        return pltpu.make_async_remote_copy(
            here, here, over_send.at[boundary, f], over_recv.at[boundary, f],
            device_id=(ta, 1 - aa), device_id_type=MESH)

    def transform(kind, f):
        before = core == kind
        for j in range(frames):
            tap = jnp.where(before, j + TAPS - 1 - f, j - f)
            used = (tap >= 0) & (tap < TAPS) & (before & (tap >= TAPS - 1 - f) | ~before & (tap < TAPS - 1))
            used = used & (before | (ta < last))
            row = pl.ds(jnp.clip(tap, 0, TAPS - 1), 1)
            weff[j : j + 1, :] = win[row, :] * jnp.where(used, 1.0, 0.0).astype(jnp.float32)
        channel_frame(signals, volts, weff, twist, mat_hi, mat_lo, parts_s, spec.at[kind * frames + f])

    def far_first(f, carry):
        transform(0, f)

        def pack(j, c):
            rows = pl.ds(pl.multiple_of((j // 2 * 4 + 2 * (1 - side) + j % 2) * wide, wide), wide)
            give[f, pl.ds(pl.multiple_of(j * wide, wide), wide), :] = spec[f, rows, :].astype(jnp.bfloat16)
            return c

        lax.fori_loop(0, half, pack, 0)
        give_far(f).start()
        return carry

    def finish(kind, f):
        def add(j, c):
            here = pl.ds(pl.multiple_of(j * wide, wide), wide)
            rows = pl.ds(pl.multiple_of(owner(kind, j) * wide, wide), wide)
            if kind == 0:
                other = take[f, here, :].astype(jnp.float32)
            else:
                other = take_wide[f, j]
            total = spec[kind * frames + f, rows, :] + other
            done.at[kind * frames + f].reshape(CH, signals)[here, :] = total.astype(jnp.bfloat16)
            return c

        lax.fori_loop(0, half, add, 0)
        over_own(kind, f).start()
        keep(kind, f).start()

        def each(n, c):
            j = pair(own_block(kind), half - 1 - n, half)
            send(kind, f, j).start()
            return c

        lax.fori_loop(0, half - 1, each, 0)

    def finish_far(f):
        give_far(f).wait_recv()
        finish(0, f)

    def forward(kind, f):
        def each(q, c):
            boundary = 2 * pair(ta // 2, q, half) + kind

            @pl.when(maker(boundary) != ta)
            def _():
                arrival(boundary, f).wait_recv()
                over(aa, boundary, f).start()

            return c

        lax.fori_loop(0, half, each, 0)

    def near_step(f, carry):
        transform(1, f)
        give_near(f).start()
        finish_far(f)
        give_near(f).wait_recv()
        finish(1, f)
        @pl.when(f > 0)
        def _():
            forward(0, f - 1)
            forward(1, f - 1)

        return carry

    lax.fori_loop(0, frames, far_first, 0)
    lax.fori_loop(0, frames, near_step, 0)
    forward(0, frames - 1)
    forward(1, frames - 1)

    def settle(f, carry):
        give_far(f).wait_send()
        give_near(f).wait_send()
        for kind in range(2):
            keep(kind, f).wait()

            def each(n, c):
                send(kind, f, pair(own_block(kind), half - 1 - n, half)).wait_send()
                return c

            lax.fori_loop(0, half - 1, each, 0)

        def crossed(boundary, c):
            over(aa, boundary, f).wait_send()
            over(1 - aa, boundary, f).wait_recv()
            return c

        lax.fori_loop(0, peers, crossed, 0)
        return carry

    lax.fori_loop(0, frames, settle, 0)


def exchange(voltages, window, signals, frames, peers):
    mat_hi, mat_lo = stage_two_matrix()
    dma = pltpu.SemaphoreType.DMA
    hbm = pl.BlockSpec(memory_space=pltpu.HBM)
    mine = CH // peers
    return pl.pallas_call(
        functools.partial(exchange_kernel, signals, frames, peers),
        out_shape=jax.ShapeDtypeStruct((2, mine, frames * peers, 2, signals), jnp.bfloat16),
        in_specs=[hbm] * 5,
        out_specs=hbm,
        scratch_shapes=[
            pltpu.VMEM((frames, signals, NFFT), jnp.bfloat16),
            pltpu.VMEM((TAPS, NFFT), jnp.float32),
            pltpu.VMEM((2, HALF + 1, INNER), jnp.float32),
            pltpu.VMEM((4 * BINS, 2 * INNER), jnp.bfloat16),
            pltpu.VMEM((4 * BINS, 2 * INNER), jnp.bfloat16),
            pltpu.VMEM((frames, NFFT), jnp.float32),
            pltpu.VMEM((HALF + 1, 2 * signals, 2 * INNER), jnp.bfloat16),
            pltpu.VMEM((2 * frames, 2 * CH, signals), jnp.float32),
            pltpu.VMEM((frames, CH, signals), jnp.bfloat16),
            pltpu.VMEM((frames, CH, signals), jnp.bfloat16),
            pltpu.VMEM((frames, peers // 2, 2 * mine, signals), jnp.float32),
            pltpu.VMEM((2 * frames, CH // 2, 2, signals), jnp.bfloat16),
            dma((4,)),
            dma((frames,)),
            dma((2 * frames,)),
            dma((2 * frames,)),
            dma((2 * frames,)),
            dma((2 * frames, peers // 2)),
            dma((peers, frames)),
            dma((peers, frames)),
            dma((peers, frames)),
        ],
        compiler_params=pltpu.CompilerParams(
            collective_id=0, has_side_effects=True, vmem_limit_bytes=62 * 1024 * 1024
        ),
    )(voltages, window, jnp.asarray(twist_table()), jnp.asarray(mat_hi), jnp.asarray(mat_lo))


def correlate_kernel(block, signals, scale, place, grid_in, out):
    side = place[0]
    rows = grid_in.shape[2]
    dims = (((0,), (0,)), ((), ()))
    even = lax.broadcasted_iota(jnp.int32, (rows, signals), 0) % 2 == 0
    for c in range(block):
        left = grid_in[side, c]
        wide = left.astype(jnp.float32)
        turned = jnp.where(even, pltpu.roll(wide, rows - 1, 0), -pltpu.roll(wide, 1, 0))
        both = jnp.concatenate([left, turned.astype(jnp.bfloat16)], axis=1)
        against = jnp.concatenate([grid_in[0, c], grid_in[1, c]], axis=1)
        res = lax.dot_general(both, against, dims, preferred_element_type=jnp.float32) * scale
        out[c, :, : 2 * signals] = res[:signals]
        out[c, :, 2 * signals :] = res[signals:]


def correlate(spectra, place, scale):
    _, channels, rows, signals = spectra.shape
    block = 16 if rows <= 128 else 8
    return pl.pallas_call(
        functools.partial(correlate_kernel, block, signals, scale),
        grid_spec=pltpu.PrefetchScalarGridSpec(
            num_scalar_prefetch=1,
            grid=(channels // block,),
            in_specs=[pl.BlockSpec((2, block, rows, signals), lambda i, p: (0, i, 0, 0))],
            out_specs=pl.BlockSpec((block, signals, 4 * signals), lambda i, p: (i, 0, 0)),
        ),
        out_shape=jax.ShapeDtypeStruct((channels, signals, 4 * signals), jnp.float32),
        compiler_params=pltpu.CompilerParams(
            dimension_semantics=("arbitrary",), vmem_limit_bytes=62 * 1024 * 1024
        ),
    )(place.astype(jnp.int32).reshape(1), spectra)


def per_device(voltages, pfb_window):
    signals, samples = voltages.shape
    frames = samples // NFFT
    peers = lax.axis_size("ta")
    assert lax.axis_size("aa") == 2 and frames == TAPS - 1 and signals == LANES
    spectra = exchange(voltages, pfb_window, signals, frames, peers)
    spectra = spectra.reshape(2, CH // peers, frames * peers * 2, signals)
    scale = 1.0 / math.sqrt(frames * peers)
    return correlate(spectra, lax.axis_index("aa"), scale)


def solution(mesh):
    return jax.shard_map(
        per_device, mesh=mesh, in_specs=(P("aa", "ta"), P()), out_specs=P("ta", "aa", None),
        check_vma=False,
    )
```
